32 devices in a mesh: surf: 8 (over z, y), pair: 4 (over x, core).
Axes of the slice: x: 2, y: 2, z: 4, core: 2. Of those that a mesh axis runs over, the one named last changes fastest.
Arguments:
- left_panel: bfloat16 [64, 4, 128, 192], P(('surf', 'pair')), may hold values from -0.5 to 0.5
- right_panel: bfloat16 [64, 4, 128, 192], P(('surf', 'pair')), may hold values from -6 to 6
- inverse: bfloat16 [64, 128, 128], P(('surf', 'pair')), may hold values from -0.5 to 0.5
- target: int32 [64, 4, 4], P(('surf', 'pair')), may hold values from 0 to 127, as said below
- blocks: float32 [128, 192, 192], P(('surf', 'pair')), may hold values from -12 to 12
- weights: bfloat16 [128, 192, 512], P('surf', None, 'pair'), may hold values from -0.109375 to 0.109375
Outputs:
- updated: float32 [128, 192, 192], P(('surf', 'pair'))
- coarse_panel: float32 [1536, 512], P('surf', 'pair')
The draws below stay inside these ranges and needn't reach their ends.
Inputs may be any that keep to these rules, and one draw needn't show every extreme that they name: target[b, k, l] = target[b, l, k]. Pair block p lies on device p // 4 of the joined axes; the block of every term lies on a device with the same index along pair as the box's device, whose index along surf differs from the box's device's by at most 2 along the closed loop of 8 tiles. From the boxes of one device at most 8 unordered neighbour pairs (k <= l) go to any one tile, and every device sends exactly 8 to some tile in every draw.
All inputs are finite; a program needn't handle non-finite values.
Results may differ from the reference program's by a relative error of at most 0.0055.
Values may be sent and summed in bfloat16 or wider, within the bound.
No kernel may reach another device: no remote copies, remote signals or barrier semaphores. Data moves between devices by JAX's collectives and lax.ppermute only.
A program may use at most 64 MiB of HBM per device.

```python
import jax
import jax.numpy as jnp
import numpy as np
from jax import lax

REDUNDANT = 128
SKEL = 192
NEIGH = 4
REACH = 2
BOX_DEV = 2
PAIR_DEV = 4
UNITS = 20
CAP = 8
NBOX = 64
NPAIR = 128
TILES = 8
TILE_PAIRS = 16
COLS = 512
N_SURF = 8
N_PAIR = 4


def pair_table():
    table = np.zeros((NEIGH, NEIGH), np.int32)
    counter = 0
    for first in range(NEIGH):
        for second in range(first, NEIGH):
            table[first, second] = counter
            table[second, first] = counter
            counter += 1
    return table


def draw_target(key, part):
    device_count = NBOX // BOX_DEV
    spots = 2 * REACH + 1
    slot_count = spots * CAP
    key_popular, key_hot, key_noise, key_order, key_block = jax.random.split(jax.random.fold_in(key, 7), 5)
    popular = jax.random.randint(key_popular, (device_count, spots), 0, 4)
    hottest = jax.random.randint(key_hot, (device_count,), 0, spots)
    slot_spot = jnp.arange(slot_count) // CAP
    bias = popular[:, slot_spot] * 4096 + (slot_spot[None, :] == hottest[:, None]).astype(jnp.int32) * 32768
    noise = jax.random.randint(key_noise, (device_count, slot_count), 0, 4096)
    scores = (bias + noise) * slot_count + jnp.arange(slot_count)[None, :]
    _, chosen = lax.top_k(scores, UNITS)
    order_keys = jax.random.randint(key_order, (device_count, UNITS), 0, 65536) * UNITS + jnp.arange(UNITS)[None, :]
    shuffle = jnp.argsort(order_keys, axis=1, stable=True)
    chosen = jnp.take_along_axis(chosen, shuffle, axis=1)
    offset = chosen // CAP - REACH
    device = jnp.arange(device_count)
    own_tile = device // N_PAIR
    pair_index = device % N_PAIR
    dest_tile = (own_tile[:, None] + offset + N_SURF) % N_SURF
    block_slot = jax.random.randint(key_block, (device_count, UNITS), 0, PAIR_DEV)
    unit_target = ((dest_tile * N_PAIR + pair_index[:, None]) * PAIR_DEV + block_slot).reshape(NBOX, UNITS // BOX_DEV)
    table = jnp.asarray(pair_table().reshape(-1))
    return unit_target[:, table].reshape(NBOX, NEIGH, NEIGH).astype(jnp.int32)


def shard_levels(stream_key, extent, shards, least, high):
    gain, own = 1.0, jax.random.fold_in(stream_key, 6)
    for axis_at, shards_of in shards:
        draws = jnp.exp(jax.random.uniform(jax.random.fold_in(own, axis_at), (shards_of,), jnp.float32, least / len(shards), high / len(shards)))
        gain = gain * jnp.repeat(draws, extent[axis_at] // shards_of).reshape([-1 if axis == axis_at else 1 for axis in range(len(extent))])
    return gain


def bell_draw(own_key, dims, deviation, limit, shards=(), dtype=jnp.bfloat16):
    entries = jax.random.normal(own_key, dims, jnp.float32) * deviation
    if len(shards) > 0:
        entries = shard_levels(own_key, dims, shards, -0.22, 0.18) * entries
    return jnp.clip(entries, min=-limit, max=limit).astype(dtype)


def setup_inputs(seed: int = 0) -> dict:
    seeds = jax.random.split(jax.random.key(seed), 7)
    left_panel = bell_draw(seeds[0], (NBOX, NEIGH, REDUNDANT, SKEL), REDUNDANT ** -0.5, 0.5, ((0, 32),))
    right_panel = bell_draw(seeds[1], (NBOX, NEIGH, REDUNDANT, SKEL), 1.0, 6.0, ((0, 32),))
    inverse = bell_draw(seeds[2], (NBOX, REDUNDANT, REDUNDANT), REDUNDANT ** -0.5, 0.5, ((0, 32),))
    target = draw_target(jax.random.fold_in(seeds[6], 71), 0)
    blocks = bell_draw(seeds[4], (NPAIR, SKEL, SKEL), 2.0, 12.0, ((0, 32),), jnp.float32)
    weights = bell_draw(seeds[5], (NPAIR, SKEL, COLS), (TILE_PAIRS * SKEL) ** -0.5, 0.109375, ((0, 8), (2, 4)))
    return dict(left_panel=left_panel, right_panel=right_panel, inverse=inverse, target=target, blocks=blocks, weights=weights)


def reference(left_panel, right_panel, inverse, target, blocks, weights):
    lower = (jnp.arange(NEIGH)[:, None] > jnp.arange(NEIGH)[None, :])[:, :, None, None]

    def eliminate(running, inputs):
        left_box, right_box, inverse_box, target_box = inputs
        solved = jnp.einsum('ij,kjc->kic', inverse_box.astype(jnp.float32), right_box.astype(jnp.float32)).astype(jnp.bfloat16)
        solved = lax.optimization_barrier(solved).astype(jnp.float32)
        products = jnp.einsum('kri,lrj->klij', left_box.astype(jnp.float32), solved).astype(jnp.bfloat16)
        products = lax.optimization_barrier(products).astype(jnp.float32)
        chosen = jnp.where(lower, jnp.swapaxes(products, 2, 3), products)
        running = running.at[target_box.reshape(-1).astype(jnp.int32)].add(-chosen.reshape(-1, SKEL, SKEL))
        return running, None

    updated, _ = lax.scan(eliminate, blocks, (left_panel, right_panel, inverse, target))
    rounded = lax.optimization_barrier(updated.astype(jnp.bfloat16)).astype(jnp.float32)
    tiled = rounded.reshape(TILES, TILE_PAIRS, SKEL, SKEL)
    tiled_weights = weights.astype(jnp.float32).reshape(TILES, TILE_PAIRS, SKEL, COLS)
    coarse_panel = jnp.einsum('tpij,tpjc->tic', tiled, tiled_weights).reshape(TILES * SKEL, COLS)
    return updated, coarse_panel
```

```python
import jax
import jax.numpy as jnp
from jax import lax
from jax.experimental import pallas as pl
from jax.experimental.pallas import tpu as pltpu
from jax.sharding import PartitionSpec as P

REACH = 2
ROLES = 2 * REACH + 1
DIRECT, FAR, OWN, NEAR, COMB = range(ROLES)
LANES = 128


def dot_nt(a, b):
    return lax.dot_general(a, b, (((1,), (1,)), ((), ())), preferred_element_type=jnp.float32)


def terms_kernel(surf_count, pair_count, lt_ref, rt_ref, inv_ref, target_ref, direct_ref, far_ref, near_ref, comb_ref, own_ref, terms, acc):
    box_count, neighbours, skeleton, _ = lt_ref.shape
    slots = own_ref.shape[0]
    tail = skeleton - LANES
    me = lax.axis_index("surf")
    even = lax.rem(me, 2) == 0
    acc[...] = jnp.zeros_like(acc)
    cells = []
    for box in range(box_count):
        inverse = inv_ref[box]
        left = [lt_ref[box, k] for k in range(neighbours)]
        solved = [dot_nt(rt_ref[box, k], inverse).astype(jnp.bfloat16) for k in range(neighbours)]
        for second in range(neighbours):
            both = jnp.concatenate([solved[second], left[second]], axis=1)
            both = jnp.concatenate([both, both[LANES:]], axis=0)
            for first in range(second + 1):
                if first == second:
                    term = dot_nt(left[first], both[:, :LANES])
                else:
                    term = dot_nt(jnp.concatenate([left[first], solved[first]], axis=1), both)
                terms[len(cells)] = term
                block = target_ref[box, first, second]
                tile = block // (slots * pair_count)
                slot = lax.rem(block, slots)
                ahead = lax.rem(tile - me + surf_count, surf_count)
                ahead = jnp.where(ahead <= REACH, ahead, ahead - surf_count)
                role = jnp.where(even, ahead, -ahead) + REACH
                cells.append(role * slots + slot)
    for unit, cell in enumerate(cells):
        acc[cell] += terms[unit]
    lane = lax.broadcasted_iota(jnp.int32, (skeleton, LANES), 1)
    for role, ref in ((FAR, far_ref), (DIRECT, direct_ref), (NEAR, near_ref), (COMB, comb_ref)):
        for slot in range(slots):
            ref[slot] = acc[role * slots + slot, :, :LANES].astype(jnp.bfloat16)
        for pair in range(slots // 2):
            low = acc[role * slots + 2 * pair, :, LANES:]
            high = acc[role * slots + 2 * pair + 1, :, LANES:]
            ref[slots + pair] = jnp.where(lane < tail, low, high).astype(jnp.bfloat16)
    own_ref[...] = acc[OWN * slots : (OWN + 1) * slots, :, :skeleton]


def update_kernel(blocks_ref, own_ref, near_ref, direct_ref, comb_ref, *refs):
    slots, skeleton, _ = blocks_ref.shape
    shifts = (len(refs) - 1) // 2
    weights = refs[:shifts]
    updated_ref = refs[shifts]
    parts = refs[shifts + 1 :]
    tail = skeleton - LANES

    def received(row):
        return near_ref[row].astype(jnp.float32) + direct_ref[row].astype(jnp.float32) + comb_ref[row].astype(jnp.float32)

    total = [None] * shifts
    for pair in range(slots // 2):
        tails = received(slots + pair)
        for half in range(2):
            slot = 2 * pair + half
            gone = jnp.concatenate([received(slot), tails[:, half * tail : (half + 1) * tail]], axis=1)
            updated = blocks_ref[slot] - own_ref[slot] - gone
            updated_ref[slot] = updated
            rounded = updated.astype(jnp.bfloat16)
            for shift in range(shifts):
                part = jnp.dot(rounded, weights[shift][slot], preferred_element_type=jnp.float32)
                total[shift] = part if total[shift] is None else total[shift] + part
    for shift in range(shifts):
        parts[shift][...] = total[shift].astype(parts[shift].dtype)


def body(left_panel, right_panel, inverse, target, blocks, weights):
    box_count, neighbours, redundant, skeleton = left_panel.shape
    surf_count = lax.axis_size("surf")
    pair_count = lax.axis_size("pair")
    slots = blocks.shape[0]
    columns = weights.shape[2]
    packed = jax.ShapeDtypeStruct((slots + slots // 2, skeleton, LANES), jnp.bfloat16)
    units = box_count * neighbours * (neighbours + 1) // 2
    vmem = pl.BlockSpec(memory_space=pltpu.VMEM)
    smem = pl.BlockSpec(memory_space=pltpu.SMEM)

    def terms_call(*refs):
        terms_kernel(surf_count, pair_count, *refs)

    direct, far, near, comb, own = pl.pallas_call(
        terms_call,
        out_shape=[packed, packed, packed, packed, jax.ShapeDtypeStruct(blocks.shape, jnp.float32)],
        in_specs=[vmem, vmem, vmem, smem],
        out_specs=[vmem] * 5,
        scratch_shapes=[
            pltpu.VMEM((units, skeleton, 2 * LANES), jnp.float32),
            pltpu.VMEM((ROLES * slots, skeleton, 2 * LANES), jnp.float32),
        ],
        name="terms",
    )(jnp.swapaxes(left_panel, 2, 3), jnp.swapaxes(right_panel, 2, 3), inverse, target)

    def send(piece, even_by, odd_by):
        moves = [(i, (i + (odd_by if i % 2 else even_by)) % surf_count) for i in range(surf_count)]
        return lax.ppermute(piece, "surf", moves)

    me = lax.axis_index("pair")
    far = send(far, 1, -1)
    direct = send(direct, -2, 2)
    near = send(near, 1, -1)
    comb = (comb.astype(jnp.float32) + far.astype(jnp.float32)).astype(jnp.bfloat16)
    comb = send(comb, 2, -2)

    panels = []
    for shift in range(pair_count):
        dest = lax.rem(me + shift, pair_count)
        mine = lax.dynamic_slice_in_dim(weights, dest * slots, slots, axis=0)
        if shift:
            mine = lax.ppermute(mine, "pair", [(i, (i + shift) % pair_count) for i in range(pair_count)])
        panels.append(mine)

    part = jax.ShapeDtypeStruct((skeleton, columns), jnp.bfloat16)
    updated, kept, *parts = pl.pallas_call(
        update_kernel,
        out_shape=[jax.ShapeDtypeStruct(blocks.shape, jnp.float32), jax.ShapeDtypeStruct((skeleton, columns), jnp.float32)] + [part] * (pair_count - 1),
        in_specs=[vmem] * (5 + pair_count),
        out_specs=[vmem] * (1 + pair_count),
        name="update",
    )(blocks, own, near, direct, comb, *panels)
    for shift, piece in enumerate(parts, 1):
        back = lax.ppermute(piece, "pair", [(i, (i - shift) % pair_count) for i in range(pair_count)])
        kept = kept + back.astype(jnp.float32)
    return (updated, kept)


def solution(mesh):
    if mesh.shape["surf"] % 2 or mesh.shape["surf"] < 2 * REACH + 1:
        raise ValueError("surf size")
    in_specs = (
        P(("surf", "pair"), None, None, None),
        P(("surf", "pair"), None, None, None),
        P(("surf", "pair"), None, None),
        P(("surf", "pair"), None, None),
        P(("surf", "pair"), None, None),
        P("surf", None, "pair"),
    )
    out_specs = (P(("surf", "pair"), None, None), P("surf", "pair"))
    return jax.shard_map(body, mesh=mesh, in_specs=in_specs, out_specs=out_specs, check_vma=False)
```

```python
import functools

import jax
import jax.numpy as jnp
from jax import lax
from jax.experimental import pallas as pl
from jax.experimental.pallas import tpu as pltpu
from jax.sharding import PartitionSpec as P

REACH = 2
ROLES = 2 * REACH + 1
DIRECT, FAR, OWN, NEAR, COMB = range(ROLES)
LANES = 128
CHUNKS = 2


def dot_nt(a, b):
    return lax.dot_general(a, b, (((1,), (1,)), ((), ())), preferred_element_type=jnp.float32)


def terms_kernel(chunk, surf_count, pair_count, lt_ref, target_ref, read_target, out_refs, terms, acc, ready):
    direct_ref, far_ref, near_ref, comb_ref, own_ref = out_refs
    box_count, neighbours, skeleton, _ = lt_ref.shape
    slots, rows, _ = own_ref.shape
    span = slice(chunk * rows, (chunk + 1) * rows)
    tail = skeleton - LANES
    me = lax.axis_index("surf")
    even = lax.rem(me, 2) == 0
    acc[...] = jnp.zeros_like(acc)
    units = []
    for box in range(box_count):
        left, solved = ready(box)
        for second in range(neighbours):
            both = jnp.concatenate([solved[second], left[second]], axis=1)
            both = jnp.concatenate([both, both[LANES:]], axis=0)
            for first in range(second + 1):
                if first == second:
                    term = dot_nt(left[first][span], both[:, :LANES])
                else:
                    term = dot_nt(jnp.concatenate([left[first][span], solved[first][span]], axis=1), both)
                terms[len(units)] = term
                units.append((box, first, second))
    read_target.wait()
    for unit, at in enumerate(units):
        block = target_ref[at]
        tile = block // (slots * pair_count)
        slot = lax.rem(block, slots)
        ahead = lax.rem(tile - me + surf_count, surf_count)
        ahead = jnp.where(ahead <= REACH, ahead, ahead - surf_count)
        role = jnp.where(even, ahead, -ahead) + REACH
        acc[role * slots + slot] += terms[unit]
    lane = lax.broadcasted_iota(jnp.int32, (rows, LANES), 1)
    for role, ref in ((DIRECT, direct_ref), (FAR, far_ref), (NEAR, near_ref), (COMB, comb_ref)):
        for slot in range(slots):
            ref[slot] = acc[role * slots + slot, :, :LANES].astype(jnp.bfloat16)
        for pair in range(slots // 2):
            low = acc[role * slots + 2 * pair, :, LANES:]
            high = acc[role * slots + 2 * pair + 1, :, LANES:]
            ref[slots + pair] = jnp.where(lane < tail, low, high).astype(jnp.bfloat16)
    own_ref[...] = acc[OWN * slots : (OWN + 1) * slots, :, :skeleton]


def first_terms(surf_count, pair_count, lt_hbm, rt_hbm, inv_hbm, weights_hbm, target_hbm, *refs):
    *refs, rt_ref, inv_ref, terms, acc, sem, weights_sem, target_ref, target_sem = refs
    out_refs, (lt_ref, solved_ref), weight_refs = refs[:ROLES], refs[ROLES : ROLES + 2], refs[ROLES + 2 :]
    box_count, neighbours = lt_ref.shape[:2]
    outer_count = pair_count // 2
    slots = weight_refs[0].shape[0]
    read_target = pltpu.make_async_copy(target_hbm, target_ref, target_sem)
    read_target.start()
    copies = []
    for box in range(box_count):
        group = []
        for hbm, ref in ((inv_hbm, inv_ref), (rt_hbm, rt_ref), (lt_hbm, lt_ref)):
            group.append(pltpu.make_async_copy(hbm.at[box], ref.at[box], sem.at[3 * box + len(group)]))
            group[-1].start()
        copies.append(group)
    me = lax.axis_index("pair")
    outer, inner = me // 2, lax.rem(me, 2)
    cuts = []
    for shift in range(outer_count):
        for half in range(2):
            dest = lax.rem(outer + shift, outer_count) * 2 + (inner if half == 0 else 1 - inner)
            if shift:
                cut = weight_refs[shift].at[pl.ds(half * slots, slots)]
            else:
                cut = weight_refs[-1 if half else 0]
            cuts.append(pltpu.make_async_copy(weights_hbm.at[pl.ds(dest * slots, slots)], cut, weights_sem.at[len(cuts)]))
            cuts[-1].start()

    def ready(box):
        for copy in copies[box]:
            copy.wait()
        inverse = inv_ref[box]
        solved = []
        for k in range(neighbours):
            solved.append(dot_nt(rt_ref[box, k], inverse).astype(jnp.bfloat16))
            solved_ref[box, k] = solved[k]
        return [lt_ref[box, k] for k in range(neighbours)], solved

    terms_kernel(0, surf_count, pair_count, lt_ref, target_ref, read_target, out_refs, terms, acc, ready)
    for copy in cuts:
        copy.wait()


def later_terms(chunk, surf_count, pair_count, lt_ref, solved_ref, target_hbm, *refs):
    *out_refs, terms, acc, target_ref, target_sem = refs
    read_target = pltpu.make_async_copy(target_hbm, target_ref, target_sem)
    read_target.start()
    neighbours = lt_ref.shape[1]

    def ready(box):
        return [lt_ref[box, k] for k in range(neighbours)], [solved_ref[box, k] for k in range(neighbours)]

    terms_kernel(chunk, surf_count, pair_count, lt_ref, target_ref, read_target, out_refs, terms, acc, ready)


def update_kernel(chunk, outer_count, *refs):
    blocks_ref, own_ref, direct_ref, near_ref, comb_ref, kept_w, peer_w = refs[:7]
    outer_w = refs[7 : 6 + outer_count]
    updated_ref, kept_ref, peer_ref, *outer_refs = refs[6 + outer_count :]
    slots, rows, skeleton = own_ref.shape
    span = slice(chunk * rows, (chunk + 1) * rows)
    tail = skeleton - LANES

    def received(row):
        return near_ref[row].astype(jnp.float32) + direct_ref[row].astype(jnp.float32) + comb_ref[row].astype(jnp.float32)

    panels = [(kept_w, 0), (peer_w, 0)]
    for shift in range(1, outer_count):
        panels += [(outer_w[shift - 1], 0), (peer_w, shift * slots)]
    total = [None] * len(panels)
    for pair in range(slots // 2):
        tails = received(slots + pair)
        for half in range(2):
            slot = 2 * pair + half
            gone = jnp.concatenate([received(slot), tails[:, half * tail : (half + 1) * tail]], axis=1)
            updated = blocks_ref[slot, span] - own_ref[slot] - gone
            updated_ref[slot] = updated
            rounded = updated.astype(jnp.bfloat16)
            for at, (panel, base) in enumerate(panels):
                part = jnp.dot(rounded, panel[base + slot], preferred_element_type=jnp.float32)
                total[at] = part if total[at] is None else total[at] + part
    kept_ref[...] = total[0]
    peer_ref[0] = total[1].astype(peer_ref.dtype)
    for shift in range(outer_count - 1):
        outer_refs[shift][...] = total[2 + 2 * shift]
        peer_ref[1 + shift] = total[3 + 2 * shift].astype(peer_ref.dtype)


def body(left_panel, right_panel, inverse, target, blocks, weights):
    box_count, neighbours, redundant, skeleton = left_panel.shape
    surf_count = lax.axis_size("surf")
    pair_count = lax.axis_size("pair")
    outer_count = pair_count // 2
    slots = blocks.shape[0]
    columns = weights.shape[2]
    rows = skeleton // CHUNKS
    units = box_count * neighbours * (neighbours + 1) // 2
    vmem = pl.BlockSpec(memory_space=pltpu.VMEM)
    hbm = pl.BlockSpec(memory_space=pltpu.HBM)

    def shape(*dims, dtype=jnp.bfloat16):
        return jax.ShapeDtypeStruct(dims, dtype)

    def to_tile(piece, even_by, odd_by):
        moves = [(i, (i + (odd_by if i % 2 else even_by)) % surf_count) for i in range(surf_count)]
        return lax.ppermute(piece, "surf", moves)

    def to_outer(piece, shift):
        moves = [(i, ((i // 2 + shift) % outer_count) * 2 + i % 2) for i in range(pair_count)]
        return lax.ppermute(piece, "pair", moves)

    def to_peer(piece):
        return lax.ppermute(piece, "pair", [(i, i ^ 1) for i in range(pair_count)])

    panels_shape = shape(box_count, neighbours, skeleton, redundant)
    packed = shape(slots + slots // 2, rows, LANES)
    pieces = [packed] * (ROLES - 1) + [shape(slots, rows, skeleton, dtype=jnp.float32)]
    cuts = [shape(slots, skeleton, columns)] + [shape(2 * slots, skeleton, columns)] * (outer_count - 1) + [shape(slots, skeleton, columns)]
    sums = [pltpu.VMEM((units, rows, 2 * LANES), jnp.float32), pltpu.VMEM((ROLES * slots, rows, 2 * LANES), jnp.float32)]
    read = [pltpu.SMEM(target.shape, target.dtype), pltpu.SemaphoreType.DMA]
    target = pltpu.with_memory_space_constraint(target, pltpu.HBM)
    direct, far, near, comb, own = ([] for _ in range(ROLES))
    lt, solved = None, None
    for chunk in range(CHUNKS):
        if chunk == 0:
            out = pl.pallas_call(
                functools.partial(first_terms, surf_count, pair_count),
                out_shape=pieces + [panels_shape, panels_shape] + cuts,
                in_specs=[hbm] * 5,
                out_specs=[vmem] * (ROLES + 2 + len(cuts)),
                scratch_shapes=[
                    pltpu.VMEM(panels_shape.shape, jnp.bfloat16),
                    pltpu.VMEM((box_count, redundant, redundant), jnp.bfloat16),
                    *sums,
                    pltpu.SemaphoreType.DMA((3 * box_count,)),
                    pltpu.SemaphoreType.DMA((pair_count,)),
                    *read,
                ],
                compiler_params=pltpu.CompilerParams(vmem_limit_bytes=16 << 20),
                name="first_terms",
            )(*(pltpu.with_memory_space_constraint(array, pltpu.HBM) for array in (jnp.swapaxes(left_panel, 2, 3), jnp.swapaxes(right_panel, 2, 3), inverse, weights)), target)
            lt, solved = out[ROLES : ROLES + 2]
            kept_w, *outer_w, peer_w = out[ROLES + 2 :]
        else:
            out = pl.pallas_call(
                functools.partial(later_terms, chunk, surf_count, pair_count),
                out_shape=pieces,
                in_specs=[vmem, vmem, hbm],
                out_specs=[vmem] * ROLES,
                scratch_shapes=sums + read,
                compiler_params=pltpu.CompilerParams(vmem_limit_bytes=16 << 20),
                name="later_terms",
            )(lt, solved, target)
        direct.append(to_tile(out[0], -2, 2))
        far.append(to_tile(out[1], 1, -1))
        near.append(to_tile(out[2], 1, -1))
        comb.append(out[3])
        own.append(out[4])

    outer_w = [to_outer(piece, shift) for shift, piece in enumerate(outer_w, 1)]
    peer_w = to_peer(jnp.concatenate([peer_w] + [piece[slots:] for piece in outer_w], axis=0))
    rest_w = [piece[:slots] for piece in outer_w]
    for chunk in range(CHUNKS):
        merged = (comb[chunk].astype(jnp.float32) + far[chunk].astype(jnp.float32)).astype(jnp.bfloat16)
        comb[chunk] = to_tile(merged, 2, -2)

    updated, panel = [], []
    for chunk in range(CHUNKS):
        fresh, kept, peer, *outer = pl.pallas_call(
            functools.partial(update_kernel, chunk, outer_count),
            out_shape=[shape(slots, rows, skeleton, dtype=jnp.float32), shape(rows, columns, dtype=jnp.float32), shape(outer_count, rows, columns)]
            + [shape(rows, columns, dtype=jnp.float32)] * (outer_count - 1),
            in_specs=[vmem] * (7 + len(rest_w)),
            out_specs=[vmem] * (2 + outer_count),
            compiler_params=pltpu.CompilerParams(vmem_limit_bytes=8 << 20),
            name="update",
        )(blocks, own[chunk], direct[chunk], near[chunk], comb[chunk], kept_w, peer_w, *rest_w)
        peer = to_peer(peer).astype(jnp.float32)
        kept = kept + peer[0]
        for shift in range(1, outer_count):
            piece = (outer[shift - 1] + peer[shift]).astype(jnp.bfloat16)
            kept = kept + to_outer(piece, -shift).astype(jnp.float32)
        updated.append(fresh)
        panel.append(kept)
    updated = jnp.concatenate(updated, axis=1)
    return (updated, jnp.concatenate(panel, axis=0))


def solution(mesh):
    if mesh.shape["surf"] % 2 or mesh.shape["surf"] < 2 * REACH + 1 or mesh.shape["pair"] % 2:
        raise ValueError("mesh sizes")
    in_specs = (
        P(("surf", "pair"), None, None, None),
        P(("surf", "pair"), None, None, None),
        P(("surf", "pair"), None, None),
        P(("surf", "pair"), None, None),
        P(("surf", "pair"), None, None),
        P("surf", None, "pair"),
    )
    out_specs = (P(("surf", "pair"), None, None), P("surf", "pair"))

    return jax.shard_map(body, mesh=mesh, in_specs=in_specs, out_specs=out_specs, check_vma=False)
```

```python
import functools

import jax
import jax.numpy as jnp
from jax import lax
from jax.experimental import pallas as pl
from jax.experimental.pallas import tpu as pltpu
from jax.sharding import PartitionSpec as P

REACH = 2
ROLES = 2 * REACH + 1
DIRECT, FAR, OWN, NEAR, COMB = range(ROLES)
LANES = 128
CHUNKS = 2


def dot_nt(a, b):
    return lax.dot_general(a, b, (((1,), (1,)), ((), ())), preferred_element_type=jnp.float32)


def terms_kernel(surf_count, pair_count, lt_hbm, rt_hbm, inv_hbm, weights_hbm, target_hbm, *refs):
    out_refs, weight_refs, refs = refs[: ROLES + 2 * (CHUNKS - 1)], refs[ROLES + 2 * (CHUNKS - 1) : -8], refs[-8:]
    lt_ref, rt_ref, inv_ref, target_ref, acc, sem, weights_sem, target_sem = refs
    direct_ref, near_ref, own_ref = out_refs[:3]
    far_refs, comb_refs = out_refs[3 : 3 + CHUNKS], out_refs[3 + CHUNKS :]
    box_count, neighbours, skeleton, _ = lt_ref.shape
    slots = own_ref.shape[0]
    outer_count = pair_count // 2
    tail = skeleton - LANES
    read_target = pltpu.make_async_copy(target_hbm, target_ref, target_sem)
    read_target.start()
    copies = []
    for box in range(box_count):
        group = []
        for hbm, ref in ((inv_hbm, inv_ref), (rt_hbm, rt_ref), (lt_hbm, lt_ref)):
            group.append(pltpu.make_async_copy(hbm.at[box], ref.at[box], sem.at[3 * box + len(group)]))
            group[-1].start()
        copies.append(group)
    pair = lax.axis_index("pair")
    outer, inner = pair // 2, lax.rem(pair, 2)
    cuts = []
    for shift in range(outer_count):
        for half in range(2):
            dest = lax.rem(outer + shift, outer_count) * 2 + (inner if half == 0 else 1 - inner)
            if shift:
                cut = weight_refs[shift].at[pl.ds(half * slots, slots)]
            else:
                cut = weight_refs[-1 if half else 0]
            cuts.append(pltpu.make_async_copy(weights_hbm.at[pl.ds(dest * slots, slots)], cut, weights_sem.at[len(cuts)]))
            cuts[-1].start()
    acc[...] = jnp.zeros_like(acc)
    me = lax.axis_index("surf")
    even = lax.rem(me, 2) == 0

    def cell(*at):
        block = target_ref[at]
        tile = block // (slots * pair_count)
        ahead = lax.rem(tile - me + surf_count, surf_count)
        ahead = jnp.where(ahead <= REACH, ahead, ahead - surf_count)
        return (jnp.where(even, ahead, -ahead) + REACH) * slots + lax.rem(block, slots)

    read_target.wait()
    for box in range(box_count):
        for copy in copies[box]:
            copy.wait()
        inverse = inv_ref[box]
        left = [lt_ref[box, k] for k in range(neighbours)]
        solved = [dot_nt(rt_ref[box, k], inverse).astype(jnp.bfloat16) for k in range(neighbours)]
        for second in range(neighbours):
            both = jnp.concatenate([solved[second], left[second]], axis=1)
            both = jnp.concatenate([both, both[LANES:]], axis=0)
            for first in range(second + 1):
                if first == second:
                    term = dot_nt(left[first], both[:, :LANES])
                else:
                    term = dot_nt(jnp.concatenate([left[first], solved[first]], axis=1), both)
                acc[cell(box, first, second)] += term
    lane = lax.broadcasted_iota(jnp.int32, (skeleton, LANES), 1)
    for role, refs in ((FAR, far_refs), (DIRECT, [direct_ref]), (COMB, comb_refs), (NEAR, [near_ref])):
        rows = skeleton // len(refs)
        for chunk, ref in enumerate(refs):
            span = slice(chunk * rows, (chunk + 1) * rows)
            for slot in range(slots):
                ref[slot] = acc[role * slots + slot, span, :LANES].astype(jnp.bfloat16)
            for two in range(slots // 2):
                low = acc[role * slots + 2 * two, span, LANES:]
                high = acc[role * slots + 2 * two + 1, span, LANES:]
                ref[slots + two] = jnp.where(lane[:rows] < tail, low, high).astype(jnp.bfloat16)
    own_ref[...] = acc[OWN * slots : (OWN + 1) * slots, :, :skeleton]
    for copy in cuts:
        copy.wait()


def update_kernel(chunk, outer_count, *refs):
    blocks_ref, own_ref, direct_ref, near_ref, comb_ref, kept_w, peer_w = refs[:7]
    outer_w = refs[7 : 6 + outer_count]
    updated_ref, kept_ref, peer_ref, *outer_refs = refs[-2 - outer_count :]
    slots, skeleton, _ = own_ref.shape
    rows = comb_ref.shape[1]
    span = slice(chunk * rows, (chunk + 1) * rows)
    tail = skeleton - LANES

    def received(row):
        return near_ref[row, span].astype(jnp.float32) + direct_ref[row, span].astype(jnp.float32) + comb_ref[row].astype(jnp.float32)

    panels = [(kept_w, 0), (peer_w, 0)]
    for shift in range(1, outer_count):
        panels += [(outer_w[shift - 1], 0), (peer_w, shift * slots)]
    total = [None] * len(panels)
    for two in range(slots // 2):
        tails = received(slots + two)
        for half in range(2):
            slot = 2 * two + half
            gone = jnp.concatenate([received(slot), tails[:, half * tail : (half + 1) * tail]], axis=1)
            updated = blocks_ref[slot, span] - own_ref[slot, span] - gone
            updated_ref[slot] = updated
            rounded = updated.astype(jnp.bfloat16)
            for at, (panel, base) in enumerate(panels):
                part = jnp.dot(rounded, panel[base + slot], preferred_element_type=jnp.float32)
                total[at] = part if total[at] is None else total[at] + part
    kept_ref[span] = total[0]
    peer_ref[0, span] = total[1].astype(peer_ref.dtype)
    for shift in range(outer_count - 1):
        outer_refs[shift][span] = total[2 + 2 * shift]
        peer_ref[1 + shift, span] = total[3 + 2 * shift].astype(peer_ref.dtype)


def body(left_panel, right_panel, inverse, target, blocks, weights):
    box_count, neighbours, redundant, skeleton = left_panel.shape
    surf_count = lax.axis_size("surf")
    pair_count = lax.axis_size("pair")
    outer_count = pair_count // 2
    slots = blocks.shape[0]
    columns = weights.shape[2]
    rows = skeleton // CHUNKS
    vmem = pl.BlockSpec(memory_space=pltpu.VMEM)
    hbm = pl.BlockSpec(memory_space=pltpu.HBM)

    def shape(*dims, dtype=jnp.bfloat16):
        return jax.ShapeDtypeStruct(dims, dtype)

    def to_tile(piece, even_by, odd_by):
        moves = [(i, (i + (odd_by if i % 2 else even_by)) % surf_count) for i in range(surf_count)]
        return lax.ppermute(piece, "surf", moves)

    def to_outer(piece, shift):
        moves = [(i, ((i // 2 + shift) % outer_count) * 2 + i % 2) for i in range(pair_count)]
        return lax.ppermute(piece, "pair", moves)

    def to_peer(piece):
        return lax.ppermute(piece, "pair", [(i, i ^ 1) for i in range(pair_count)])

    panels_shape = (box_count, neighbours, skeleton, redundant)
    full = shape(slots + slots // 2, skeleton, LANES)
    part = shape(slots + slots // 2, rows, LANES)
    cuts = [shape(slots, skeleton, columns)] + [shape(2 * slots, skeleton, columns)] * (outer_count - 1) + [shape(slots, skeleton, columns)]
    out_shape = [full, full, shape(*blocks.shape, dtype=jnp.float32)] + [part] * (2 * CHUNKS) + cuts
    args = (jnp.swapaxes(left_panel, 2, 3), jnp.swapaxes(right_panel, 2, 3), inverse, weights, target)
    direct, near, own, *out = pl.pallas_call(
        functools.partial(terms_kernel, surf_count, pair_count),
        out_shape=out_shape,
        in_specs=[hbm] * len(args),
        out_specs=[vmem] * len(out_shape),
        scratch_shapes=[
            pltpu.VMEM(panels_shape, jnp.bfloat16),
            pltpu.VMEM(panels_shape, jnp.bfloat16),
            pltpu.VMEM((box_count, redundant, redundant), jnp.bfloat16),
            pltpu.SMEM(target.shape, target.dtype),
            pltpu.VMEM((ROLES * slots, skeleton, 2 * LANES), jnp.float32),
            pltpu.SemaphoreType.DMA((3 * box_count,)),
            pltpu.SemaphoreType.DMA((pair_count,)),
            pltpu.SemaphoreType.DMA,
        ],
        compiler_params=pltpu.CompilerParams(vmem_limit_bytes=20 << 20),
        name="terms",
    )(*(pltpu.with_memory_space_constraint(array, pltpu.HBM) for array in args))
    far, comb, (kept_w, *outer_w, peer_w) = out[:CHUNKS], out[CHUNKS : 2 * CHUNKS], out[2 * CHUNKS :]

    far = [to_tile(piece, 1, -1) for piece in far]
    direct = to_tile(direct, -2, 2)
    near = to_tile(near, 1, -1)
    outer_w = [to_outer(piece, shift) for shift, piece in enumerate(outer_w, 1)]
    peer_w = to_peer(jnp.concatenate([peer_w] + [piece[slots:] for piece in outer_w], axis=0))
    outer_w = [piece[:slots] for piece in outer_w]
    for chunk in range(CHUNKS):
        merged = (comb[chunk].astype(jnp.float32) + far[chunk].astype(jnp.float32)).astype(jnp.bfloat16)
        comb[chunk] = to_tile(merged, 2, -2)

    updated, sums = [], []
    for chunk in range(CHUNKS):
        inputs = [blocks, own, direct, near, comb[chunk], kept_w, peer_w, *outer_w]
        fresh, *sums = pl.pallas_call(
            functools.partial(update_kernel, chunk, outer_count),
            out_shape=[shape(slots, rows, skeleton, dtype=jnp.float32), shape(skeleton, columns, dtype=jnp.float32), shape(outer_count, skeleton, columns)]
            + [shape(skeleton, columns, dtype=jnp.float32)] * (outer_count - 1),
            in_specs=[vmem] * (len(inputs) + len(sums)),
            out_specs=[vmem] * (2 + outer_count),
            input_output_aliases={len(inputs) + at: 1 + at for at in range(len(sums))},
            compiler_params=pltpu.CompilerParams(vmem_limit_bytes=8 << 20),
            name="update",
        )(*inputs, *sums)
        updated.append(fresh)
    kept, peer, *outer = sums
    peer = to_peer(peer).astype(jnp.float32)
    kept = kept + peer[0]
    for shift in range(1, outer_count):
        piece = (outer[shift - 1] + peer[shift]).astype(jnp.bfloat16)
        kept = kept + to_outer(piece, -shift).astype(jnp.float32)
    return (jnp.concatenate(updated, axis=1), kept)


def solution(mesh):
    if mesh.shape["surf"] % 2 or mesh.shape["surf"] < 2 * REACH + 1 or mesh.shape["pair"] % 2:
        raise ValueError("mesh sizes")
    in_specs = (
        P(("surf", "pair"), None, None, None),
        P(("surf", "pair"), None, None, None),
        P(("surf", "pair"), None, None),
        P(("surf", "pair"), None, None),
        P(("surf", "pair"), None, None),
        P("surf", None, "pair"),
    )
    out_specs = (P(("surf", "pair"), None, None), P("surf", "pair"))

    return jax.shard_map(body, mesh=mesh, in_specs=in_specs, out_specs=out_specs, check_vma=False)
```

```python
import functools

import jax
import jax.numpy as jnp
from jax import lax
from jax.experimental import pallas as pl
from jax.experimental.pallas import tpu as pltpu
from jax.sharding import PartitionSpec as P

REACH = 2
ROLES = 2 * REACH + 1
DIRECT, FAR, OWN, NEAR, COMB = range(ROLES)
LANES = 128
CHUNKS = 2


def chunk_rows(skeleton):
    cuts = [skeleton * at // CHUNKS // 16 * 16 for at in range(CHUNKS)] + [skeleton]
    return list(zip(cuts, cuts[1:]))


def dot_nt(a, b):
    return lax.dot_general(a, b, (((1,), (1,)), ((), ())), preferred_element_type=jnp.float32)


def terms_kernel(surf_count, pair_count, lt_hbm, rt_hbm, inv_hbm, weights_hbm, target_hbm, *refs):
    out_refs, weight_refs, refs = refs[: ROLES + 2 * (CHUNKS - 1)], refs[ROLES + 2 * (CHUNKS - 1) : -8], refs[-8:]
    lt_ref, rt_ref, inv_ref, target_ref, acc, sem, weights_sem, target_sem = refs
    direct_ref, near_ref, own_ref = out_refs[:3]
    far_refs, comb_refs = out_refs[3 : 3 + CHUNKS], out_refs[3 + CHUNKS :]
    box_count, neighbours, skeleton, _ = lt_ref.shape
    slots = own_ref.shape[0]
    outer_count = pair_count // 2
    tail = skeleton - LANES
    read_target = pltpu.make_async_copy(target_hbm, target_ref, target_sem)
    read_target.start()
    copies = [
        pltpu.make_async_copy(hbm, ref, sem.at[at]) for at, (hbm, ref) in enumerate(((inv_hbm, inv_ref), (rt_hbm, rt_ref), (lt_hbm, lt_ref)))
    ]
    for copy in copies:
        copy.start()
    pair = lax.axis_index("pair")
    outer, inner = pair // 2, lax.rem(pair, 2)
    cuts = []
    for shift in range(outer_count):
        for half in range(2):
            dest = lax.rem(outer + shift, outer_count) * 2 + (inner if half == 0 else 1 - inner)
            if shift:
                cut = weight_refs[shift].at[pl.ds(half * slots, slots)]
            else:
                cut = weight_refs[-1 if half else 0]
            cuts.append(pltpu.make_async_copy(weights_hbm.at[pl.ds(dest * slots, slots)], cut, weights_sem.at[len(cuts)]))
            cuts[-1].start()
    acc[...] = jnp.zeros_like(acc)
    me = lax.axis_index("surf")
    even = lax.rem(me, 2) == 0

    def cell(*at):
        block = target_ref[at]
        tile = block // (slots * pair_count)
        ahead = lax.rem(tile - me + surf_count, surf_count)
        ahead = jnp.where(ahead <= REACH, ahead, ahead - surf_count)
        return (jnp.where(even, ahead, -ahead) + REACH) * slots + lax.rem(block, slots)

    copies[0].wait()
    copies[1].wait()
    solves = [[dot_nt(rt_ref[box, k], inv_ref[box]).astype(jnp.bfloat16) for k in range(neighbours)] for box in range(box_count)]
    copies[2].wait()
    read_target.wait()
    for box in range(box_count):
        left, solved = [lt_ref[box, k] for k in range(neighbours)], solves[box]
        for second in range(neighbours):
            both = jnp.concatenate([solved[second], left[second]], axis=1)
            both = jnp.concatenate([both, both[LANES:]], axis=0)
            for first in range(second + 1):
                if first == second:
                    term = dot_nt(left[first], both[:, :LANES])
                else:
                    term = dot_nt(jnp.concatenate([left[first], solved[first]], axis=1), both)
                acc[cell(box, first, second)] += term
    lane = lax.broadcasted_iota(jnp.int32, (skeleton, LANES), 1)
    for role, refs in ((FAR, far_refs), (DIRECT, [direct_ref]), (COMB, comb_refs), (NEAR, [near_ref])):
        spans = chunk_rows(skeleton) if len(refs) == CHUNKS else [(0, skeleton)]
        for (start, stop), ref in zip(spans, refs):
            span, rows = slice(start, stop), stop - start
            for slot in range(slots):
                ref[slot] = acc[role * slots + slot, span, :LANES].astype(jnp.bfloat16)
            for two in range(slots // 2):
                low = acc[role * slots + 2 * two, span, LANES:]
                high = acc[role * slots + 2 * two + 1, span, LANES:]
                ref[slots + two] = jnp.where(lane[:rows] < tail, low, high).astype(jnp.bfloat16)
    own_ref[...] = acc[OWN * slots : (OWN + 1) * slots, :, :skeleton]
    for copy in cuts:
        copy.wait()


def update_kernel(chunk, outer_count, *refs):
    blocks_ref, own_ref, direct_ref, near_ref, comb_ref, kept_w, peer_w = refs[:7]
    outer_w = refs[7 : 6 + outer_count]
    updated_ref, kept_ref, *part_refs = refs[-1 - 2 * outer_count :]
    slots, skeleton, _ = own_ref.shape
    span = slice(*chunk_rows(skeleton)[chunk])
    tail = skeleton - LANES

    def received(row):
        return near_ref[row, span].astype(jnp.float32) + direct_ref[row, span].astype(jnp.float32) + comb_ref[row].astype(jnp.float32)

    panels = [(kept_w, 0), (peer_w, 0)]
    for shift in range(1, outer_count):
        panels += [(outer_w[shift - 1], 0), (peer_w, shift * slots)]
    total = [None] * len(panels)
    for two in range(slots // 2):
        tails = received(slots + two)
        for half in range(2):
            slot = 2 * two + half
            gone = jnp.concatenate([received(slot), tails[:, half * tail : (half + 1) * tail]], axis=1)
            updated = blocks_ref[slot, span] - own_ref[slot, span] - gone
            updated_ref[slot] = updated
            rounded = updated.astype(jnp.bfloat16)
            for at, (panel, base) in enumerate(panels):
                part = jnp.dot(rounded, panel[base + slot], preferred_element_type=jnp.float32)
                total[at] = part if total[at] is None else total[at] + part
    kept_ref[span] = total[0]
    for at, ref in enumerate(part_refs, 1):
        ref[span] = total[at].astype(ref.dtype)


def body(left_panel, right_panel, inverse, target, blocks, weights):
    box_count, neighbours, redundant, skeleton = left_panel.shape
    surf_count = lax.axis_size("surf")
    pair_count = lax.axis_size("pair")
    outer_count = pair_count // 2
    slots = blocks.shape[0]
    columns = weights.shape[2]
    rows = [stop - start for start, stop in chunk_rows(skeleton)]
    vmem = pl.BlockSpec(memory_space=pltpu.VMEM)
    hbm = pl.BlockSpec(memory_space=pltpu.HBM)

    def shape(*dims, dtype=jnp.bfloat16):
        return jax.ShapeDtypeStruct(dims, dtype)

    def to_tile(piece, even_by, odd_by):
        moves = [(i, (i + (odd_by if i % 2 else even_by)) % surf_count) for i in range(surf_count)]
        return lax.ppermute(piece, "surf", moves)

    def to_outer(piece, shift):
        moves = [(i, ((i // 2 + shift) % outer_count) * 2 + i % 2) for i in range(pair_count)]
        return lax.ppermute(piece, "pair", moves)

    def to_peer(piece):
        return lax.ppermute(piece, "pair", [(i, i ^ 1) for i in range(pair_count)])

    panels_shape = (box_count, neighbours, skeleton, redundant)
    full = shape(slots + slots // 2, skeleton, LANES)
    parts = [shape(slots + slots // 2, count, LANES) for count in rows]
    cuts = [shape(slots, skeleton, columns)] + [shape(2 * slots, skeleton, columns)] * (outer_count - 1) + [shape(slots, skeleton, columns)]
    out_shape = [full, full, shape(*blocks.shape, dtype=jnp.float32)] + 2 * parts + cuts
    args = (jnp.swapaxes(left_panel, 2, 3), jnp.swapaxes(right_panel, 2, 3), inverse, weights, target)
    direct, near, own, *out = pl.pallas_call(
        functools.partial(terms_kernel, surf_count, pair_count),
        out_shape=out_shape,
        in_specs=[hbm] * len(args),
        out_specs=[vmem] * len(out_shape),
        scratch_shapes=[
            pltpu.VMEM(panels_shape, jnp.bfloat16),
            pltpu.VMEM(panels_shape, jnp.bfloat16),
            pltpu.VMEM((box_count, redundant, redundant), jnp.bfloat16),
            pltpu.SMEM(target.shape, target.dtype),
            pltpu.VMEM((ROLES * slots, skeleton, 2 * LANES), jnp.float32),
            pltpu.SemaphoreType.DMA((3,)),
            pltpu.SemaphoreType.DMA((pair_count,)),
            pltpu.SemaphoreType.DMA,
        ],
        compiler_params=pltpu.CompilerParams(vmem_limit_bytes=20 << 20),
        name="terms",
    )(*(pltpu.with_memory_space_constraint(array, pltpu.HBM) for array in args))
    far, comb, (kept_w, *outer_w, peer_w) = out[:CHUNKS], out[CHUNKS : 2 * CHUNKS], out[2 * CHUNKS :]

    far = [to_tile(piece, 1, -1) for piece in far]
    direct = to_tile(direct, -2, 2)
    near = to_tile(near, 1, -1)
    outer_w = [to_outer(piece, shift) for shift, piece in enumerate(outer_w, 1)]
    peer_w = to_peer(jnp.concatenate([peer_w] + [piece[slots:] for piece in outer_w], axis=0))
    outer_w = [piece[:slots] for piece in outer_w]
    for chunk in range(CHUNKS):
        merged = (comb[chunk].astype(jnp.float32) + far[chunk].astype(jnp.float32)).astype(jnp.bfloat16)
        comb[chunk] = to_tile(merged, 2, -2)

    updated, sums = [], []
    for chunk in range(CHUNKS):
        inputs = [blocks, own, direct, near, comb[chunk], kept_w, peer_w, *outer_w]
        fresh, *sums = pl.pallas_call(
            functools.partial(update_kernel, chunk, outer_count),
            out_shape=[shape(slots, rows[chunk], skeleton, dtype=jnp.float32), shape(skeleton, columns, dtype=jnp.float32)]
            + [shape(skeleton, columns)] * (pair_count - 1),
            in_specs=[vmem] * (len(inputs) + len(sums)),
            out_specs=[vmem] * (1 + pair_count),
            input_output_aliases={len(inputs) + at: 1 + at for at in range(len(sums))},
            compiler_params=pltpu.CompilerParams(vmem_limit_bytes=8 << 20),
            name="update",
        )(*inputs, *sums)
        updated.append(fresh)
    kept, *parts = sums
    for at, piece in enumerate(parts, 1):
        shift, cross = divmod(at, 2)
        moves = [(i, ((i // 2 - shift) % outer_count) * 2 + (i % 2 ^ cross)) for i in range(pair_count)]
        kept = kept + lax.ppermute(piece, "pair", moves).astype(jnp.float32)
    return (jnp.concatenate(updated, axis=1), kept)


def solution(mesh):
    if mesh.shape["surf"] % 2 or mesh.shape["surf"] < 2 * REACH + 1 or mesh.shape["pair"] % 2:
        raise ValueError("mesh sizes")
    in_specs = (
        P(("surf", "pair"), None, None, None),
        P(("surf", "pair"), None, None, None),
        P(("surf", "pair"), None, None),
        P(("surf", "pair"), None, None),
        P(("surf", "pair"), None, None),
        P("surf", None, "pair"),
    )
    out_specs = (P(("surf", "pair"), None, None), P("surf", "pair"))

    return jax.shard_map(body, mesh=mesh, in_specs=in_specs, out_specs=out_specs, check_vma=False)
```

```python
import functools

import jax
import jax.numpy as jnp
from jax import lax
from jax.experimental import pallas as pl
from jax.experimental.pallas import tpu as pltpu
from jax.sharding import PartitionSpec as P

REACH = 2
ROLES = 2 * REACH + 1
DIRECT, FAR, OWN, NEAR, COMB = range(ROLES)
LANES = 128
CHUNKS = 2


def chunk_rows(skeleton):
    cuts = [skeleton * at // CHUNKS // 16 * 16 for at in range(CHUNKS)] + [skeleton]
    return list(zip(cuts, cuts[1:]))


def dot_nt(a, b):
    return lax.dot_general(a, b, (((1,), (1,)), ((), ())), preferred_element_type=jnp.float32)


def terms_kernel(surf_count, pair_count, lt_hbm, rt_hbm, inv_hbm, weights_hbm, target_hbm, *refs):
    out_refs, weight_refs, refs = refs[: ROLES + 2 * (CHUNKS - 1)], refs[ROLES + 2 * (CHUNKS - 1) : -8], refs[-8:]
    lt_ref, rt_ref, inv_ref, target_ref, acc, sem, weights_sem, target_sem = refs
    direct_ref, near_ref, own_ref = out_refs[:3]
    far_refs, comb_refs = out_refs[3 : 3 + CHUNKS], out_refs[3 + CHUNKS :]
    box_count, neighbours, skeleton, _ = lt_ref.shape
    slots = own_ref.shape[0]
    outer_count = pair_count // 2
    tail = skeleton - LANES
    read_target = pltpu.make_async_copy(target_hbm, target_ref, target_sem)
    read_target.start()
    copies = [
        pltpu.make_async_copy(hbm, ref, sem.at[at]) for at, (hbm, ref) in enumerate(((inv_hbm, inv_ref), (rt_hbm, rt_ref), (lt_hbm, lt_ref)))
    ]
    for copy in copies:
        copy.start()
    pair = lax.axis_index("pair")
    outer, inner = pair // 2, lax.rem(pair, 2)
    cuts = []
    for shift in range(outer_count):
        for half in range(2):
            dest = lax.rem(outer + shift, outer_count) * 2 + (inner if half == 0 else 1 - inner)
            if shift:
                cut = weight_refs[shift].at[pl.ds(half * slots, slots)]
            else:
                cut = weight_refs[-1 if half else 0]
            cuts.append(pltpu.make_async_copy(weights_hbm.at[pl.ds(dest * slots, slots)], cut, weights_sem.at[len(cuts)]))
            cuts[-1].start()
    acc[...] = jnp.zeros_like(acc)
    me = lax.axis_index("surf")
    even = lax.rem(me, 2) == 0

    def cell(*at):
        block = target_ref[at]
        tile = block // (slots * pair_count)
        ahead = lax.rem(tile - me + surf_count, surf_count)
        ahead = jnp.where(ahead <= REACH, ahead, ahead - surf_count)
        return (jnp.where(even, ahead, -ahead) + REACH) * slots + lax.rem(block, slots)

    copies[0].wait()
    copies[1].wait()
    solves = [[dot_nt(rt_ref[box, k], inv_ref[box]).astype(jnp.bfloat16) for k in range(neighbours)] for box in range(box_count)]
    copies[2].wait()
    read_target.wait()
    for box in range(box_count):
        left, solved = [lt_ref[box, k] for k in range(neighbours)], solves[box]
        for second in range(neighbours):
            both = jnp.concatenate([solved[second], left[second]], axis=1)
            both = jnp.concatenate([both, both[LANES:]], axis=0)
            for first in range(second + 1):
                if first == second:
                    term = dot_nt(left[first], both[:, :LANES])
                else:
                    term = dot_nt(jnp.concatenate([left[first], solved[first]], axis=1), both)
                acc[cell(box, first, second)] += term
    lane = lax.broadcasted_iota(jnp.int32, (skeleton, LANES), 1)
    for role, refs in ((FAR, far_refs), (DIRECT, [direct_ref]), (COMB, comb_refs), (NEAR, [near_ref])):
        spans = chunk_rows(skeleton) if len(refs) == CHUNKS else [(0, skeleton)]
        for (start, stop), ref in zip(spans, refs):
            span, rows = slice(start, stop), stop - start
            for slot in range(slots):
                ref[slot] = acc[role * slots + slot, span, :LANES].astype(jnp.bfloat16)
            for two in range(slots // 2):
                low = acc[role * slots + 2 * two, span, LANES:]
                high = acc[role * slots + 2 * two + 1, span, LANES:]
                ref[slots + two] = jnp.where(lane[:rows] < tail, low, high).astype(jnp.bfloat16)
    own_ref[...] = acc[OWN * slots : (OWN + 1) * slots, :, :skeleton]
    for copy in cuts:
        copy.wait()


def update_kernel(chunk, outer_count, *refs):
    blocks_ref, own_ref, direct_ref, near_ref, comb_ref, kept_w, peer_w = refs[:7]
    outer_w = refs[7 : 6 + outer_count]
    updated_ref, kept_ref, *part_refs = refs[-1 - 2 * outer_count :]
    slots, skeleton, _ = own_ref.shape
    span = slice(*chunk_rows(skeleton)[chunk])
    tail = skeleton - LANES

    def received(row):
        return near_ref[row, span].astype(jnp.float32) + direct_ref[row, span].astype(jnp.float32) + comb_ref[row].astype(jnp.float32)

    panels = [((kept_w, 0), (peer_w, 0))]
    panels += [((outer_w[shift - 1], 0), (peer_w, shift * slots)) for shift in range(1, outer_count)]
    total = [None] * len(panels)
    for two in range(slots // 2):
        tails = received(slots + two)
        for half in range(2):
            slot = 2 * two + half
            gone = jnp.concatenate([received(slot), tails[:, half * tail : (half + 1) * tail]], axis=1)
            updated = blocks_ref[slot, span] - own_ref[slot, span] - gone
            updated_ref[slot] = updated
            rounded = updated.astype(jnp.bfloat16)
            for at, pair in enumerate(panels):
                panel = jnp.concatenate([ref[base + slot] for ref, base in pair], axis=1)
                part = jnp.dot(rounded, panel, preferred_element_type=jnp.float32)
                total[at] = part if total[at] is None else total[at] + part
    columns = kept_ref.shape[-1]
    for at, ref in enumerate((kept_ref, *part_refs)):
        ref[span] = total[at // 2][:, at % 2 * columns : (at % 2 + 1) * columns].astype(ref.dtype)


def body(left_panel, right_panel, inverse, target, blocks, weights):
    box_count, neighbours, redundant, skeleton = left_panel.shape
    surf_count = lax.axis_size("surf")
    pair_count = lax.axis_size("pair")
    outer_count = pair_count // 2
    slots = blocks.shape[0]
    columns = weights.shape[2]
    rows = [stop - start for start, stop in chunk_rows(skeleton)]
    vmem = pl.BlockSpec(memory_space=pltpu.VMEM)
    hbm = pl.BlockSpec(memory_space=pltpu.HBM)

    def shape(*dims, dtype=jnp.bfloat16):
        return jax.ShapeDtypeStruct(dims, dtype)

    def to_tile(piece, even_by, odd_by):
        moves = [(i, (i + (odd_by if i % 2 else even_by)) % surf_count) for i in range(surf_count)]
        return lax.ppermute(piece, "surf", moves)

    def to_outer(piece, shift):
        moves = [(i, ((i // 2 + shift) % outer_count) * 2 + i % 2) for i in range(pair_count)]
        return lax.ppermute(piece, "pair", moves)

    def to_peer(piece):
        return lax.ppermute(piece, "pair", [(i, i ^ 1) for i in range(pair_count)])

    panels_shape = (box_count, neighbours, skeleton, redundant)
    full = shape(slots + slots // 2, skeleton, LANES)
    parts = [shape(slots + slots // 2, count, LANES) for count in rows]
    cuts = [shape(slots, skeleton, columns)] + [shape(2 * slots, skeleton, columns)] * (outer_count - 1) + [shape(slots, skeleton, columns)]
    out_shape = [full, full, shape(*blocks.shape, dtype=jnp.float32)] + 2 * parts + cuts
    args = (jnp.swapaxes(left_panel, 2, 3), jnp.swapaxes(right_panel, 2, 3), inverse, weights, target)
    direct, near, own, *out = pl.pallas_call(
        functools.partial(terms_kernel, surf_count, pair_count),
        out_shape=out_shape,
        in_specs=[hbm] * len(args),
        out_specs=[vmem] * len(out_shape),
        scratch_shapes=[
            pltpu.VMEM(panels_shape, jnp.bfloat16),
            pltpu.VMEM(panels_shape, jnp.bfloat16),
            pltpu.VMEM((box_count, redundant, redundant), jnp.bfloat16),
            pltpu.SMEM(target.shape, target.dtype),
            pltpu.VMEM((ROLES * slots, skeleton, 2 * LANES), jnp.float32),
            pltpu.SemaphoreType.DMA((3,)),
            pltpu.SemaphoreType.DMA((pair_count,)),
            pltpu.SemaphoreType.DMA,
        ],
        compiler_params=pltpu.CompilerParams(vmem_limit_bytes=20 << 20),
        name="terms",
    )(*(pltpu.with_memory_space_constraint(array, pltpu.HBM) for array in args))
    far, comb, (kept_w, *outer_w, peer_w) = out[:CHUNKS], out[CHUNKS : 2 * CHUNKS], out[2 * CHUNKS :]

    far = [to_tile(piece, 1, -1) for piece in far]
    direct = to_tile(direct, -2, 2)
    near = to_tile(near, 1, -1)
    outer_w = [to_outer(piece, shift) for shift, piece in enumerate(outer_w, 1)]
    peer_w = to_peer(jnp.concatenate([peer_w] + [piece[slots:] for piece in outer_w], axis=0))
    outer_w = [piece[:slots] for piece in outer_w]
    for chunk in range(CHUNKS):
        merged = (comb[chunk].astype(jnp.float32) + far[chunk].astype(jnp.float32)).astype(jnp.bfloat16)
        comb[chunk] = to_tile(merged, 2, -2)

    updated, sums = [], []
    for chunk in range(CHUNKS):
        inputs = [blocks, own, direct, near, comb[chunk], kept_w, peer_w, *outer_w]
        fresh, *sums = pl.pallas_call(
            functools.partial(update_kernel, chunk, outer_count),
            out_shape=[shape(slots, rows[chunk], skeleton, dtype=jnp.float32), shape(skeleton, columns, dtype=jnp.float32)]
            + [shape(skeleton, columns)] * (pair_count - 1),
            in_specs=[vmem] * (len(inputs) + len(sums)),
            out_specs=[vmem] * (1 + pair_count),
            input_output_aliases={len(inputs) + at: 1 + at for at in range(len(sums))},
            compiler_params=pltpu.CompilerParams(vmem_limit_bytes=8 << 20),
            name="update",
        )(*inputs, *sums)
        updated.append(fresh)
    kept, *parts = sums
    for at, piece in enumerate(parts, 1):
        shift, cross = divmod(at, 2)
        moves = [(i, ((i // 2 - shift) % outer_count) * 2 + (i % 2 ^ cross)) for i in range(pair_count)]
        kept = kept + lax.ppermute(piece, "pair", moves).astype(jnp.float32)
    return (jnp.concatenate(updated, axis=1), kept)


def solution(mesh):
    if mesh.shape["surf"] % 2 or mesh.shape["surf"] < 2 * REACH + 1 or mesh.shape["pair"] % 2:
        raise ValueError("mesh sizes")
    in_specs = (
        P(("surf", "pair"), None, None, None),
        P(("surf", "pair"), None, None, None),
        P(("surf", "pair"), None, None),
        P(("surf", "pair"), None, None),
        P(("surf", "pair"), None, None),
        P("surf", None, "pair"),
    )
    out_specs = (P(("surf", "pair"), None, None), P("surf", "pair"))

    return jax.shard_map(body, mesh=mesh, in_specs=in_specs, out_specs=out_specs, check_vma=False)
```

```python
import functools

import jax
import jax.numpy as jnp
from jax import lax
from jax.experimental import pallas as pl
from jax.experimental.pallas import tpu as pltpu
from jax.sharding import PartitionSpec as P

REACH = 2
ROLES = 2 * REACH + 1
DIRECT, FAR, OWN, NEAR, COMB = range(ROLES)
LANES = 128
CHUNKS = 2


def chunk_rows(skeleton):
    cuts = [skeleton * at // CHUNKS // 16 * 16 for at in range(CHUNKS)] + [skeleton]
    return list(zip(cuts, cuts[1:]))


def dot_nt(a, b):
    return lax.dot_general(a, b, (((1,), (1,)), ((), ())), preferred_element_type=jnp.float32)


def pack(acc, role, refs):
    skeleton = acc.shape[1]
    slots = acc.shape[0] // ROLES
    spans = chunk_rows(skeleton) if len(refs) == CHUNKS else [(0, skeleton)]
    for (start, stop), ref in zip(spans, refs):
        for slot in range(slots):
            ref[slot] = acc[role * slots + slot, start:stop, :LANES].astype(jnp.bfloat16)
        lane = lax.broadcasted_iota(jnp.int32, (stop - start, LANES), 1)
        for two in range(slots // 2):
            low = acc[role * slots + 2 * two, start:stop, LANES:]
            high = acc[role * slots + 2 * two + 1, start:stop, LANES:]
            ref[slots + two] = jnp.where(lane < skeleton - LANES, low, high).astype(jnp.bfloat16)


def terms_kernel(surf_count, pair_count, lt_hbm, rt_hbm, inv_hbm, weights_hbm, target_hbm, *refs):
    acc, direct_ref, *refs = refs
    far_refs, weight_refs, refs = refs[:CHUNKS], refs[CHUNKS:-7], refs[-7:]
    lt_ref, rt_ref, inv_ref, target_ref, sem, weights_sem, target_sem = refs
    box_count, neighbours, skeleton = lt_ref.shape[:3]
    slots = acc.shape[0] // ROLES
    outer_count = pair_count // 2
    read_target = pltpu.make_async_copy(target_hbm, target_ref, target_sem)
    read_target.start()
    copies = [
        pltpu.make_async_copy(hbm, ref, sem.at[at]) for at, (hbm, ref) in enumerate(((inv_hbm, inv_ref), (rt_hbm, rt_ref), (lt_hbm, lt_ref)))
    ]
    for copy in copies:
        copy.start()
    pair = lax.axis_index("pair")
    outer, inner = pair // 2, lax.rem(pair, 2)
    cuts = []
    for shift in range(outer_count):
        for half in range(2):
            dest = lax.rem(outer + shift, outer_count) * 2 + (inner if half == 0 else 1 - inner)
            if shift:
                cut = weight_refs[shift].at[pl.ds(half * slots, slots)]
            else:
                cut = weight_refs[-1 if half else 0]
            cuts.append(pltpu.make_async_copy(weights_hbm.at[pl.ds(dest * slots, slots)], cut, weights_sem.at[len(cuts)]))
            cuts[-1].start()
    acc[...] = jnp.zeros_like(acc)
    me = lax.axis_index("surf")
    even = lax.rem(me, 2) == 0

    def cell(*at):
        block = target_ref[at]
        tile = block // (slots * pair_count)
        ahead = lax.rem(tile - me + surf_count, surf_count)
        ahead = jnp.where(ahead <= REACH, ahead, ahead - surf_count)
        return (jnp.where(even, ahead, -ahead) + REACH) * slots + lax.rem(block, slots)

    copies[0].wait()
    copies[1].wait()
    solves = [[dot_nt(rt_ref[box, k], inv_ref[box]).astype(jnp.bfloat16) for k in range(neighbours)] for box in range(box_count)]
    copies[2].wait()
    read_target.wait()
    for box in range(box_count):
        left, solved = [lt_ref[box, k] for k in range(neighbours)], solves[box]
        for second in range(neighbours):
            both = jnp.concatenate([solved[second], left[second]], axis=1)
            both = jnp.concatenate([both, both[LANES:]], axis=0)
            rows = [
                jnp.concatenate([left[first], solved[first] if first != second else jnp.zeros_like(solved[first])], axis=1)
                for first in range(second + 1)
            ]
            product = dot_nt(jnp.concatenate(rows, axis=0), both)
            for first in range(second + 1):
                acc[cell(box, first, second)] += product[first * skeleton : (first + 1) * skeleton]
    pack(acc, FAR, far_refs)
    pack(acc, DIRECT, [direct_ref])
    for copy in cuts:
        copy.wait()


def pack_kernel(acc, near_ref, own_ref, *comb_refs):
    slots, skeleton, _ = own_ref.shape
    pack(acc, NEAR, [near_ref])
    pack(acc, COMB, comb_refs)
    own_ref[...] = acc[OWN * slots : (OWN + 1) * slots, :, :skeleton]


def update_kernel(chunk, outer_count, *refs):
    blocks_ref, own_ref, direct_ref, near_ref, comb_ref, kept_w, peer_w = refs[:7]
    outer_w = refs[7 : 6 + outer_count]
    updated_ref, kept_ref, *part_refs = refs[-1 - 2 * outer_count :]
    slots, skeleton, _ = own_ref.shape
    span = slice(*chunk_rows(skeleton)[chunk])
    tail = skeleton - LANES

    def received(row):
        return near_ref[row, span].astype(jnp.float32) + direct_ref[row, span].astype(jnp.float32) + comb_ref[row].astype(jnp.float32)

    panels = [((kept_w, 0), (peer_w, 0))]
    panels += [((outer_w[shift - 1], 0), (peer_w, shift * slots)) for shift in range(1, outer_count)]
    total = [None] * len(panels)
    for two in range(slots // 2):
        tails = received(slots + two)
        for half in range(2):
            slot = 2 * two + half
            gone = jnp.concatenate([received(slot), tails[:, half * tail : (half + 1) * tail]], axis=1)
            updated = blocks_ref[slot, span] - own_ref[slot, span] - gone
            updated_ref[slot] = updated
            rounded = updated.astype(jnp.bfloat16)
            for at, pair in enumerate(panels):
                panel = jnp.concatenate([ref[base + slot] for ref, base in pair], axis=1)
                part = jnp.dot(rounded, panel, preferred_element_type=jnp.float32)
                total[at] = part if total[at] is None else total[at] + part
    columns = kept_ref.shape[-1]
    for at, ref in enumerate((kept_ref, *part_refs)):
        ref[span] = total[at // 2][:, at % 2 * columns : (at % 2 + 1) * columns].astype(ref.dtype)


def body(left_panel, right_panel, inverse, target, blocks, weights):
    box_count, neighbours, redundant, skeleton = left_panel.shape
    surf_count = lax.axis_size("surf")
    pair_count = lax.axis_size("pair")
    outer_count = pair_count // 2
    slots = blocks.shape[0]
    columns = weights.shape[2]
    rows = [stop - start for start, stop in chunk_rows(skeleton)]
    vmem = pl.BlockSpec(memory_space=pltpu.VMEM)
    hbm = pl.BlockSpec(memory_space=pltpu.HBM)

    def shape(*dims, dtype=jnp.bfloat16):
        return jax.ShapeDtypeStruct(dims, dtype)

    def to_tile(piece, even_by, odd_by):
        moves = [(i, (i + (odd_by if i % 2 else even_by)) % surf_count) for i in range(surf_count)]
        return lax.ppermute(piece, "surf", moves)

    def to_outer(piece, shift):
        moves = [(i, ((i // 2 + shift) % outer_count) * 2 + i % 2) for i in range(pair_count)]
        return lax.ppermute(piece, "pair", moves)

    def to_peer(piece):
        return lax.ppermute(piece, "pair", [(i, i ^ 1) for i in range(pair_count)])

    panels_shape = (box_count, neighbours, skeleton, redundant)
    full = shape(slots + slots // 2, skeleton, LANES)
    parts = [shape(slots + slots // 2, count, LANES) for count in rows]
    cuts = [shape(slots, skeleton, columns)] + [shape(2 * slots, skeleton, columns)] * (outer_count - 1) + [shape(slots, skeleton, columns)]
    totals = shape(ROLES * slots, skeleton, 2 * LANES, dtype=jnp.float32)
    out_shape = [totals, full, *parts, *cuts]
    args = (jnp.swapaxes(left_panel, 2, 3), jnp.swapaxes(right_panel, 2, 3), inverse, weights, target)
    totals, direct, *out = pl.pallas_call(
        functools.partial(terms_kernel, surf_count, pair_count),
        out_shape=out_shape,
        in_specs=[hbm] * len(args),
        out_specs=[vmem] * len(out_shape),
        scratch_shapes=[
            pltpu.VMEM(panels_shape, jnp.bfloat16),
            pltpu.VMEM(panels_shape, jnp.bfloat16),
            pltpu.VMEM((box_count, redundant, redundant), jnp.bfloat16),
            pltpu.SMEM(target.shape, target.dtype),
            pltpu.SemaphoreType.DMA((3,)),
            pltpu.SemaphoreType.DMA((pair_count,)),
            pltpu.SemaphoreType.DMA,
        ],
        compiler_params=pltpu.CompilerParams(vmem_limit_bytes=20 << 20),
        name="terms",
    )(*(pltpu.with_memory_space_constraint(array, pltpu.HBM) for array in args))
    far, (kept_w, *outer_w, peer_w) = out[:CHUNKS], out[CHUNKS:]
    near, own, *comb = pl.pallas_call(
        pack_kernel,
        out_shape=[full, shape(*blocks.shape, dtype=jnp.float32), *parts],
        in_specs=[vmem],
        out_specs=[vmem] * (2 + CHUNKS),
        compiler_params=pltpu.CompilerParams(vmem_limit_bytes=4 << 20),
        name="pack",
    )(totals)

    far = [to_tile(piece, 1, -1) for piece in far]
    direct = to_tile(direct, -2, 2)
    near = to_tile(near, 1, -1)
    outer_w = [to_outer(piece, shift) for shift, piece in enumerate(outer_w, 1)]
    peer_w = to_peer(jnp.concatenate([peer_w] + [piece[slots:] for piece in outer_w], axis=0))
    outer_w = [piece[:slots] for piece in outer_w]
    for chunk in range(CHUNKS):
        merged = (comb[chunk].astype(jnp.float32) + far[chunk].astype(jnp.float32)).astype(jnp.bfloat16)
        comb[chunk] = to_tile(merged, 2, -2)

    updated, sums = [], []
    for chunk in range(CHUNKS):
        inputs = [blocks, own, direct, near, comb[chunk], kept_w, peer_w, *outer_w]
        fresh, *sums = pl.pallas_call(
            functools.partial(update_kernel, chunk, outer_count),
            out_shape=[shape(slots, rows[chunk], skeleton, dtype=jnp.float32), shape(skeleton, columns, dtype=jnp.float32)]
            + [shape(skeleton, columns)] * (pair_count - 1),
            in_specs=[vmem] * (len(inputs) + len(sums)),
            out_specs=[vmem] * (1 + pair_count),
            input_output_aliases={len(inputs) + at: 1 + at for at in range(len(sums))},
            compiler_params=pltpu.CompilerParams(vmem_limit_bytes=8 << 20),
            name="update",
        )(*inputs, *sums)
        updated.append(fresh)
    kept, *parts = sums
    for at, piece in enumerate(parts, 1):
        shift, cross = divmod(at, 2)
        moves = [(i, ((i // 2 - shift) % outer_count) * 2 + (i % 2 ^ cross)) for i in range(pair_count)]
        kept = kept + lax.ppermute(piece, "pair", moves).astype(jnp.float32)
    return (jnp.concatenate(updated, axis=1), kept)


def solution(mesh):
    if mesh.shape["surf"] % 2 or mesh.shape["surf"] < 2 * REACH + 1 or mesh.shape["pair"] % 2:
        raise ValueError("mesh sizes")
    in_specs = (
        P(("surf", "pair"), None, None, None),
        P(("surf", "pair"), None, None, None),
        P(("surf", "pair"), None, None),
        P(("surf", "pair"), None, None),
        P(("surf", "pair"), None, None),
        P("surf", None, "pair"),
    )
    out_specs = (P(("surf", "pair"), None, None), P("surf", "pair"))

    return jax.shard_map(body, mesh=mesh, in_specs=in_specs, out_specs=out_specs, check_vma=False)
```

```python
import functools

import jax
import jax.numpy as jnp
from jax import lax
from jax.experimental import pallas as pl
from jax.experimental.pallas import tpu as pltpu
from jax.sharding import PartitionSpec as P

REACH = 2
ROLES = 2 * REACH + 1
DIRECT, FAR, OWN, NEAR, COMB = range(ROLES)
LANES = 128
CHUNKS = 2


def chunk_rows(skeleton):
    cuts = [skeleton * at // CHUNKS // 16 * 16 for at in range(CHUNKS)] + [skeleton]
    return list(zip(cuts, cuts[1:]))


def dot_nt(a, b):
    return lax.dot_general(a, b, (((1,), (1,)), ((), ())), preferred_element_type=jnp.float32)


def pack(acc, role, refs):
    skeleton = acc.shape[1]
    slots = acc.shape[0] // ROLES
    spans = chunk_rows(skeleton) if len(refs) == CHUNKS else [(0, skeleton)]
    for (start, stop), ref in zip(spans, refs):
        for slot in range(slots):
            ref[slot] = acc[role * slots + slot, start:stop, :LANES].astype(jnp.bfloat16)
        lane = lax.broadcasted_iota(jnp.int32, (stop - start, LANES), 1)
        for two in range(slots // 2):
            low = acc[role * slots + 2 * two, start:stop, LANES:]
            high = acc[role * slots + 2 * two + 1, start:stop, LANES:]
            ref[slots + two] = jnp.where(lane < skeleton - LANES, low, high).astype(jnp.bfloat16)


def terms_kernel(surf_count, pair_count, lt_hbm, rt_hbm, inv_hbm, weights_hbm, target_hbm, *refs):
    acc, direct_ref, *refs = refs
    far_refs, weight_refs, refs = refs[:CHUNKS], refs[CHUNKS:-7], refs[-7:]
    lt_ref, rt_ref, inv_ref, target_ref, sem, weights_sem, target_sem = refs
    box_count, neighbours, skeleton = lt_ref.shape[:3]
    slots = acc.shape[0] // ROLES
    outer_count = pair_count // 2
    read_target = pltpu.make_async_copy(target_hbm, target_ref, target_sem)
    read_target.start()
    copies = [
        pltpu.make_async_copy(hbm, ref, sem.at[at]) for at, (hbm, ref) in enumerate(((inv_hbm, inv_ref), (rt_hbm, rt_ref), (lt_hbm, lt_ref)))
    ]
    for copy in copies:
        copy.start()
    pair = lax.axis_index("pair")
    outer, inner = pair // 2, lax.rem(pair, 2)
    cuts = []
    for shift in range(outer_count):
        for half in range(2):
            dest = lax.rem(outer + shift, outer_count) * 2 + (inner if half == 0 else 1 - inner)
            if shift:
                cut = weight_refs[shift].at[pl.ds(half * slots, slots)]
            else:
                cut = weight_refs[-1 if half else 0]
            cuts.append(pltpu.make_async_copy(weights_hbm.at[pl.ds(dest * slots, slots)], cut, weights_sem.at[len(cuts)]))
            cuts[-1].start()
    acc[...] = jnp.zeros_like(acc)
    me = lax.axis_index("surf")
    even = lax.rem(me, 2) == 0

    def cell(*at):
        block = target_ref[at]
        tile = block // (slots * pair_count)
        ahead = lax.rem(tile - me + surf_count, surf_count)
        ahead = jnp.where(ahead <= REACH, ahead, ahead - surf_count)
        return (jnp.where(even, ahead, -ahead) + REACH) * slots + lax.rem(block, slots)

    copies[0].wait()
    copies[1].wait()
    solves = [[dot_nt(rt_ref[box, k], inv_ref[box]).astype(jnp.bfloat16) for k in range(neighbours)] for box in range(box_count)]
    copies[2].wait()
    read_target.wait()
    for box in range(box_count):
        left, solved = [lt_ref[box, k] for k in range(neighbours)], solves[box]
        for second in range(neighbours):
            both = jnp.concatenate([solved[second], left[second]], axis=1)
            both = jnp.concatenate([both, both[LANES:]], axis=0)
            rows = [
                jnp.concatenate([left[first], solved[first] if first != second else jnp.zeros_like(solved[first])], axis=1)
                for first in range(second + 1)
            ]
            product = dot_nt(jnp.concatenate(rows, axis=0), both)
            for first in range(second + 1):
                acc[cell(box, first, second)] += product[first * skeleton : (first + 1) * skeleton]
    pack(acc, FAR, far_refs)
    pack(acc, DIRECT, [direct_ref])
    for copy in cuts:
        copy.wait()


def pack_kernel(acc, near_ref, own_ref, *comb_refs):
    slots, skeleton, _ = own_ref.shape
    pack(acc, NEAR, [near_ref])
    pack(acc, COMB, comb_refs)
    own_ref[...] = acc[OWN * slots : (OWN + 1) * slots, :, :skeleton]


def update_kernel(chunk, outer_count, *refs):
    blocks_ref, own_ref, direct_ref, near_ref, comb_ref, kept_w, peer_w = refs[:7]
    outer_w = refs[7 : 6 + outer_count]
    updated_ref, kept_ref, *part_refs = refs[-1 - 2 * outer_count :]
    slots, skeleton, _ = own_ref.shape
    span = slice(*chunk_rows(skeleton)[chunk])
    tail = skeleton - LANES

    def received(row):
        return near_ref[row, span].astype(jnp.float32) + direct_ref[row, span].astype(jnp.float32) + comb_ref[row].astype(jnp.float32)

    panels = [((kept_w, 0), (peer_w, 0))]
    panels += [((outer_w[shift - 1], 0), (peer_w, shift * slots)) for shift in range(1, outer_count)]
    total = [None] * len(panels)
    for two in range(slots // 2):
        tails = received(slots + two)
        for half in range(2):
            slot = 2 * two + half
            gone = jnp.concatenate([received(slot), tails[:, half * tail : (half + 1) * tail]], axis=1)
            updated = blocks_ref[slot, span] - own_ref[slot, span] - gone
            updated_ref[slot] = updated
            rounded = updated.astype(jnp.bfloat16)
            for at, pair in enumerate(panels):
                panel = jnp.concatenate([ref[base + slot] for ref, base in pair], axis=1)
                part = jnp.dot(rounded, panel, preferred_element_type=jnp.float32)
                total[at] = part if total[at] is None else total[at] + part
    columns = kept_ref.shape[-1]
    for at, ref in enumerate((kept_ref, *part_refs)):
        ref[span] = total[at // 2][:, at % 2 * columns : (at % 2 + 1) * columns].astype(ref.dtype)


def body(left_panel, right_panel, inverse, target, blocks, weights):
    box_count, neighbours, redundant, skeleton = left_panel.shape
    surf_count = lax.axis_size("surf")
    pair_count = lax.axis_size("pair")
    outer_count = pair_count // 2
    slots = blocks.shape[0]
    columns = weights.shape[2]
    rows = [stop - start for start, stop in chunk_rows(skeleton)]
    vmem = pl.BlockSpec(memory_space=pltpu.VMEM)
    hbm = pl.BlockSpec(memory_space=pltpu.HBM)

    def shape(*dims, dtype=jnp.bfloat16):
        return jax.ShapeDtypeStruct(dims, dtype)

    def to_tile(piece, even_by, odd_by):
        moves = [(i, (i + (odd_by if i % 2 else even_by)) % surf_count) for i in range(surf_count)]
        return lax.ppermute(piece, "surf", moves)

    def to_outer(piece, shift):
        moves = [(i, ((i // 2 + shift) % outer_count) * 2 + i % 2) for i in range(pair_count)]
        return lax.ppermute(piece, "pair", moves)

    def to_peer(piece):
        return lax.ppermute(piece, "pair", [(i, i ^ 1) for i in range(pair_count)])

    panels_shape = (box_count, neighbours, skeleton, redundant)
    full = shape(slots + slots // 2, skeleton, LANES)
    parts = [shape(slots + slots // 2, count, LANES) for count in rows]
    cuts = [shape(slots, skeleton, columns)] + [shape(2 * slots, skeleton, columns)] * (outer_count - 1) + [shape(slots, skeleton, columns)]
    totals = shape(ROLES * slots, skeleton, 2 * LANES, dtype=jnp.float32)
    out_shape = [totals, full, *parts, *cuts]
    args = (jnp.swapaxes(left_panel, 2, 3), jnp.swapaxes(right_panel, 2, 3), inverse, weights, target)
    totals, direct, *out = pl.pallas_call(
        functools.partial(terms_kernel, surf_count, pair_count),
        out_shape=out_shape,
        in_specs=[hbm] * len(args),
        out_specs=[vmem] * len(out_shape),
        scratch_shapes=[
            pltpu.VMEM(panels_shape, jnp.bfloat16),
            pltpu.VMEM(panels_shape, jnp.bfloat16),
            pltpu.VMEM((box_count, redundant, redundant), jnp.bfloat16),
            pltpu.SMEM(target.shape, target.dtype),
            pltpu.SemaphoreType.DMA((3,)),
            pltpu.SemaphoreType.DMA((pair_count,)),
            pltpu.SemaphoreType.DMA,
        ],
        compiler_params=pltpu.CompilerParams(vmem_limit_bytes=20 << 20),
        name="terms",
    )(*(pltpu.with_memory_space_constraint(array, pltpu.HBM) for array in args))
    far, (kept_w, *outer_w, peer_w) = out[:CHUNKS], out[CHUNKS:]
    near, own, *comb = pl.pallas_call(
        pack_kernel,
        out_shape=[full, shape(*blocks.shape, dtype=jnp.float32), *parts],
        in_specs=[vmem],
        out_specs=[vmem] * (2 + CHUNKS),
        compiler_params=pltpu.CompilerParams(vmem_limit_bytes=4 << 20),
        name="pack",
    )(totals)

    far = [to_tile(piece, 1, -1) for piece in far]
    direct = to_tile(direct, -2, 2)
    near = to_tile(near, 1, -1)
    outer_w = [to_outer(piece, shift) for shift, piece in enumerate(outer_w, 1)]
    peer_w = to_peer(jnp.concatenate([peer_w] + [piece[slots:] for piece in outer_w], axis=0))
    outer_w = [piece[:slots] for piece in outer_w]
    for chunk in range(CHUNKS):
        merged = (comb[chunk].astype(jnp.float32) + far[chunk].astype(jnp.float32)).astype(jnp.bfloat16)
        comb[chunk] = to_tile(merged, 2, -2)

    updated, sums = [], []
    for chunk in range(CHUNKS):
        inputs = [blocks, own, direct, near, comb[chunk], kept_w, peer_w, *outer_w]
        fresh, *sums = pl.pallas_call(
            functools.partial(update_kernel, chunk, outer_count),
            out_shape=[shape(slots, rows[chunk], skeleton, dtype=jnp.float32), shape(skeleton, columns, dtype=jnp.float32)]
            + [shape(skeleton, columns)] * (pair_count - 1),
            in_specs=[vmem] * (len(inputs) + len(sums)),
            out_specs=[vmem] * (1 + pair_count),
            input_output_aliases={len(inputs) + at: 1 + at for at in range(len(sums))},
            compiler_params=pltpu.CompilerParams(vmem_limit_bytes=8 << 20),
            name="update",
        )(*inputs, *sums)
        updated.append(fresh)
        if chunk == 0:
            early = [to_peer(sums[2 * shift + 1][: rows[0]]) for shift in range(1, outer_count)]
    kept, *parts = sums
    for at, piece in enumerate(parts, 1):
        shift, cross = divmod(at, 2)
        moves = [(i, ((i // 2 - shift) % outer_count) * 2 + (i % 2 ^ cross)) for i in range(pair_count)]
        if shift and cross:
            piece = piece[rows[0] :]
        elif shift:
            first = piece[: rows[0]].astype(jnp.float32) + early[shift - 1].astype(jnp.float32)
            piece = jnp.concatenate([first.astype(piece.dtype), piece[rows[0] :]], axis=0)
        back = lax.ppermute(piece, "pair", moves).astype(jnp.float32)
        kept = kept + jnp.pad(back, ((skeleton - back.shape[0], 0), (0, 0)))
    return (jnp.concatenate(updated, axis=1), kept)


def solution(mesh):
    if mesh.shape["surf"] % 2 or mesh.shape["surf"] < 2 * REACH + 1 or mesh.shape["pair"] % 2:
        raise ValueError("mesh sizes")
    in_specs = (
        P(("surf", "pair"), None, None, None),
        P(("surf", "pair"), None, None, None),
        P(("surf", "pair"), None, None),
        P(("surf", "pair"), None, None),
        P(("surf", "pair"), None, None),
        P("surf", None, "pair"),
    )
    out_specs = (P(("surf", "pair"), None, None), P("surf", "pair"))

    return jax.shard_map(body, mesh=mesh, in_specs=in_specs, out_specs=out_specs, check_vma=False)
```

```python
import functools

import jax
import jax.numpy as jnp
from jax import lax
from jax.experimental import pallas as pl
from jax.experimental.pallas import tpu as pltpu
from jax.sharding import PartitionSpec as P

REACH = 2
ROLES = 2 * REACH + 1
DIRECT, FAR, OWN, NEAR, COMB = range(ROLES)
LANES = 128
CHUNKS = 2


def chunk_rows(skeleton):
    cuts = [skeleton * at // CHUNKS // 16 * 16 for at in range(CHUNKS)] + [skeleton]
    return list(zip(cuts, cuts[1:]))


def dot_nt(a, b):
    return lax.dot_general(a, b, (((1,), (1,)), ((), ())), preferred_element_type=jnp.float32)


def pack(acc, role, refs):
    skeleton = acc.shape[1]
    slots = acc.shape[0] // ROLES
    spans = chunk_rows(skeleton) if len(refs) == CHUNKS else [(0, skeleton)]
    for (start, stop), ref in zip(spans, refs):
        for slot in range(slots):
            ref[slot] = acc[role * slots + slot, start:stop, :LANES].astype(jnp.bfloat16)
        lane = lax.broadcasted_iota(jnp.int32, (stop - start, LANES), 1)
        for two in range(slots // 2):
            low = acc[role * slots + 2 * two, start:stop, LANES:]
            high = acc[role * slots + 2 * two + 1, start:stop, LANES:]
            ref[slots + two] = jnp.where(lane < skeleton - LANES, low, high).astype(jnp.bfloat16)


def terms_kernel(surf_count, pair_count, lt_hbm, rt_hbm, inv_hbm, weights_hbm, target_hbm, *refs):
    acc, direct_ref, *refs = refs
    far_refs, weight_refs, refs = refs[:CHUNKS], refs[CHUNKS:-7], refs[-7:]
    lt_ref, rt_ref, inv_ref, target_ref, sem, weights_sem, target_sem = refs
    box_count, neighbours, skeleton = lt_ref.shape[:3]
    slots = acc.shape[0] // ROLES
    outer_count = pair_count // 2
    read_target = pltpu.make_async_copy(target_hbm, target_ref, target_sem)
    read_target.start()
    copies = [
        pltpu.make_async_copy(hbm, ref, sem.at[at]) for at, (hbm, ref) in enumerate(((inv_hbm, inv_ref), (rt_hbm, rt_ref), (lt_hbm, lt_ref)))
    ]
    for copy in copies:
        copy.start()
    pair = lax.axis_index("pair")
    outer, inner = pair // 2, lax.rem(pair, 2)
    cuts = []
    for shift in range(outer_count):
        for half in range(2):
            dest = lax.rem(outer + shift, outer_count) * 2 + (inner if half == 0 else 1 - inner)
            if shift:
                cut = weight_refs[shift].at[pl.ds(half * slots, slots)]
            else:
                cut = weight_refs[-1 if half else 0]
            cuts.append(pltpu.make_async_copy(weights_hbm.at[pl.ds(dest * slots, slots)], cut, weights_sem.at[len(cuts)]))
            cuts[-1].start()
    acc[...] = jnp.zeros_like(acc)
    me = lax.axis_index("surf")
    even = lax.rem(me, 2) == 0

    def cell(*at):
        block = target_ref[at]
        tile = block // (slots * pair_count)
        ahead = lax.rem(tile - me + surf_count, surf_count)
        ahead = jnp.where(ahead <= REACH, ahead, ahead - surf_count)
        return (jnp.where(even, ahead, -ahead) + REACH) * slots + lax.rem(block, slots)

    copies[0].wait()
    copies[1].wait()
    solves = [[dot_nt(rt_ref[box, k], inv_ref[box]).astype(jnp.bfloat16) for k in range(neighbours)] for box in range(box_count)]
    copies[2].wait()
    read_target.wait()
    for box in range(box_count):
        left, solved = [lt_ref[box, k] for k in range(neighbours)], solves[box]
        for second in range(neighbours):
            both = jnp.concatenate([solved[second], left[second]], axis=1)
            both = jnp.concatenate([both, both[LANES:]], axis=0)
            rows = [
                jnp.concatenate([left[first], solved[first] if first != second else jnp.zeros_like(solved[first])], axis=1)
                for first in range(second + 1)
            ]
            product = dot_nt(jnp.concatenate(rows, axis=0), both)
            for first in range(second + 1):
                acc[cell(box, first, second)] += product[first * skeleton : (first + 1) * skeleton]
    pack(acc, FAR, far_refs)
    pack(acc, DIRECT, [direct_ref])
    for copy in cuts:
        copy.wait()


def pack_kernel(acc, near_ref, own_ref, *comb_refs):
    slots, skeleton, _ = own_ref.shape
    pack(acc, NEAR, [near_ref])
    pack(acc, COMB, comb_refs)
    own_ref[...] = acc[OWN * slots : (OWN + 1) * slots, :, :skeleton]


def update_kernel(chunk, outer_count, *refs):
    count = 7 if chunk == 0 else 4
    *whole_refs, comb_ref, kept_w, peer_w = refs[:count]
    outer_w = refs[count : count + outer_count - 1]
    updated_ref, kept_ref, *part_refs = refs[-1 - 2 * outer_count :]
    slots, skeleton, _ = whole_refs[0].shape
    span = slice(*chunk_rows(skeleton)[chunk])
    tail = skeleton - LANES

    def unpack(read, two, half):
        tails = read(slots + two)[:, half * tail : (half + 1) * tail]
        return jnp.concatenate([read(2 * two + half), tails], axis=1)

    def remaining(two, half, where):
        slot = 2 * two + half
        if chunk:
            return whole_refs[0][slot, where]
        blocks_ref, own_ref, direct_ref, near_ref = whole_refs
        both = unpack(lambda row: near_ref[row, where].astype(jnp.float32) + direct_ref[row, where].astype(jnp.float32), two, half)
        return blocks_ref[slot, where] - own_ref[slot, where] - both

    panels = [((kept_w, 0), (peer_w, 0))]
    panels += [((outer_w[shift - 1], 0), (peer_w, shift * slots)) for shift in range(1, outer_count)]
    total = [None] * len(panels)
    for two in range(slots // 2):
        for half in range(2):
            slot = 2 * two + half
            updated = remaining(two, half, span) - unpack(lambda row: comb_ref[row].astype(jnp.float32), two, half)
            updated_ref[slot] = updated
            rounded = updated.astype(jnp.bfloat16)
            for at, pair in enumerate(panels):
                panel = jnp.concatenate([ref[base + slot] for ref, base in pair], axis=1)
                part = jnp.dot(rounded, panel, preferred_element_type=jnp.float32)
                total[at] = part if total[at] is None else total[at] + part
    if chunk == 0:
        rest = slice(span.stop, skeleton)
        for slot in range(slots):
            refs[-2 - 2 * outer_count][slot, rest] = remaining(slot // 2, slot % 2, rest)
    columns = kept_ref.shape[-1]
    for at, ref in enumerate((kept_ref, *part_refs)):
        ref[span] = total[at // 2][:, at % 2 * columns : (at % 2 + 1) * columns].astype(ref.dtype)


def body(left_panel, right_panel, inverse, target, blocks, weights):
    box_count, neighbours, redundant, skeleton = left_panel.shape
    surf_count = lax.axis_size("surf")
    pair_count = lax.axis_size("pair")
    outer_count = pair_count // 2
    slots = blocks.shape[0]
    columns = weights.shape[2]
    rows = [stop - start for start, stop in chunk_rows(skeleton)]
    vmem = pl.BlockSpec(memory_space=pltpu.VMEM)
    hbm = pl.BlockSpec(memory_space=pltpu.HBM)

    def shape(*dims, dtype=jnp.bfloat16):
        return jax.ShapeDtypeStruct(dims, dtype)

    def to_tile(piece, even_by, odd_by):
        moves = [(i, (i + (odd_by if i % 2 else even_by)) % surf_count) for i in range(surf_count)]
        return lax.ppermute(piece, "surf", moves)

    def to_outer(piece, shift):
        moves = [(i, ((i // 2 + shift) % outer_count) * 2 + i % 2) for i in range(pair_count)]
        return lax.ppermute(piece, "pair", moves)

    def to_peer(piece):
        return lax.ppermute(piece, "pair", [(i, i ^ 1) for i in range(pair_count)])

    panels_shape = (box_count, neighbours, skeleton, redundant)
    full = shape(slots + slots // 2, skeleton, LANES)
    parts = [shape(slots + slots // 2, count, LANES) for count in rows]
    cuts = [shape(slots, skeleton, columns)] + [shape(2 * slots, skeleton, columns)] * (outer_count - 1) + [shape(slots, skeleton, columns)]
    totals = shape(ROLES * slots, skeleton, 2 * LANES, dtype=jnp.float32)
    out_shape = [totals, full, *parts, *cuts]
    args = (jnp.swapaxes(left_panel, 2, 3), jnp.swapaxes(right_panel, 2, 3), inverse, weights, target)
    totals, direct, *out = pl.pallas_call(
        functools.partial(terms_kernel, surf_count, pair_count),
        out_shape=out_shape,
        in_specs=[hbm] * len(args),
        out_specs=[vmem] * len(out_shape),
        scratch_shapes=[
            pltpu.VMEM(panels_shape, jnp.bfloat16),
            pltpu.VMEM(panels_shape, jnp.bfloat16),
            pltpu.VMEM((box_count, redundant, redundant), jnp.bfloat16),
            pltpu.SMEM(target.shape, target.dtype),
            pltpu.SemaphoreType.DMA((3,)),
            pltpu.SemaphoreType.DMA((pair_count,)),
            pltpu.SemaphoreType.DMA,
        ],
        compiler_params=pltpu.CompilerParams(vmem_limit_bytes=20 << 20),
        name="terms",
    )(*(pltpu.with_memory_space_constraint(array, pltpu.HBM) for array in args))
    far, (kept_w, *outer_w, peer_w) = out[:CHUNKS], out[CHUNKS:]
    near, own, *comb = pl.pallas_call(
        pack_kernel,
        out_shape=[full, shape(*blocks.shape, dtype=jnp.float32), *parts],
        in_specs=[vmem],
        out_specs=[vmem] * (2 + CHUNKS),
        compiler_params=pltpu.CompilerParams(vmem_limit_bytes=4 << 20),
        name="pack",
    )(totals)

    far = [to_tile(piece, 1, -1) for piece in far]
    direct = to_tile(direct, -2, 2)
    near = to_tile(near, 1, -1)
    outer_w = [to_outer(piece, shift) for shift, piece in enumerate(outer_w, 1)]
    peer_w = to_peer(jnp.concatenate([peer_w] + [piece[slots:] for piece in outer_w], axis=0))
    outer_w = [piece[:slots] for piece in outer_w]
    for chunk in range(CHUNKS):
        merged = (comb[chunk].astype(jnp.float32) + far[chunk].astype(jnp.float32)).astype(jnp.bfloat16)
        comb[chunk] = to_tile(merged, 2, -2)

    updated, sums, base = [], [], None
    for chunk in range(CHUNKS):
        inputs = [*([base] if chunk else [blocks, own, direct, near]), comb[chunk], kept_w, peer_w, *outer_w]
        extra = [] if chunk else [shape(*blocks.shape, dtype=jnp.float32)]
        out = pl.pallas_call(
            functools.partial(update_kernel, chunk, outer_count),
            out_shape=extra + [shape(slots, rows[chunk], skeleton, dtype=jnp.float32), shape(skeleton, columns, dtype=jnp.float32)]
            + [shape(skeleton, columns)] * (pair_count - 1),
            in_specs=[vmem] * (len(inputs) + len(sums)),
            out_specs=[vmem] * (len(extra) + 1 + pair_count),
            input_output_aliases={len(inputs) + at: 1 + at for at in range(len(sums))},
            compiler_params=pltpu.CompilerParams(vmem_limit_bytes=8 << 20),
            name="update",
        )(*inputs, *sums)
        base = base if chunk else out[0]
        fresh, *sums = out[len(extra) :]
        updated.append(fresh)
    kept, *parts = sums
    for at, piece in enumerate(parts, 1):
        shift, cross = divmod(at, 2)
        moves = [(i, ((i // 2 - shift) % outer_count) * 2 + (i % 2 ^ cross)) for i in range(pair_count)]
        kept = kept + lax.ppermute(piece, "pair", moves).astype(jnp.float32)
    return (jnp.concatenate(updated, axis=1), kept)


def solution(mesh):
    if mesh.shape["surf"] % 2 or mesh.shape["surf"] < 2 * REACH + 1 or mesh.shape["pair"] % 2:
        raise ValueError("mesh sizes")
    in_specs = (
        P(("surf", "pair"), None, None, None),
        P(("surf", "pair"), None, None, None),
        P(("surf", "pair"), None, None),
        P(("surf", "pair"), None, None),
        P(("surf", "pair"), None, None),
        P("surf", None, "pair"),
    )
    out_specs = (P(("surf", "pair"), None, None), P("surf", "pair"))

    return jax.shard_map(body, mesh=mesh, in_specs=in_specs, out_specs=out_specs, check_vma=False)
```
